256 devices in a mesh: occ: 4 (over z_lo), vir: 64 (over y, x, z_hi, core).
Axes of the slice: x: 4, y: 4, z: 8 (z_hi: 2, z_lo: 4; z = z_hi * 4 + z_lo), core: 2. Of those that a mesh axis runs over, the one named last changes fastest.
Arguments:
- amplitudes: bfloat16 [352, 32768], P('occ', 'vir'), may hold values from -6 to 6
- integrals: bfloat16 [32768, 32768], P('vir', 'occ'), may hold values from -0.25 to 0.25
- labels: int32 [256], replicated, may hold values from 0 to 7
- slot_tile: int32 [256], replicated, may hold values from 0 to 255, each once
Outputs:
- residual: float32 [352, 32768], P(None, ('occ', 'vir'))
The draws below stay inside these ranges and needn't reach their ends.
Inputs may be any that keep to these rules, and one draw needn't show every extreme that they name: `slot_tile`: each tile appears in exactly one slot.
All inputs are finite; a program needn't handle non-finite values.
Results may differ from the reference program's by a relative error of at most 0.0003.
Values may be sent and summed in bfloat16 or wider, within the bound.
A program may use at most 128 MiB of HBM per device.

```python
import math
import jax
import jax.numpy as jnp
import numpy as np
from jax import lax

TILE = 128
NSYM = 8
NT = 256
PAIRS = 352


def touch_ends(drawn, own_key, smallest, top_value):
    longest = drawn.shape.index(max(drawn.shape))
    spots = []
    for shift in (0, 1):
        where = [jax.random.randint(jax.random.fold_in(own_key, axis), (), 0, length) for axis, length in enumerate(drawn.shape)]
        where[longest] = (where[longest] + shift) % drawn.shape[longest]
        spots.append(tuple(where))
    return drawn.at[spots[0]].set(smallest).at[spots[1]].set(top_value)


def spiked(result, rng, source, target, shards_of, factor):
    def block_of(axis_at):
        return (jnp.arange(result.shape[axis_at]) // (result.shape[axis_at] // shards_of)).reshape((-1,) + (1,) * (result.ndim - 1 - axis_at))

    one_side = jax.random.permutation(rng, shards_of)[block_of(target)]
    far = (block_of(target) + shards_of // 2) % shards_of
    return jnp.where((block_of(source) == one_side) | (block_of(source) == far), factor * result, result)


def block_levels(stream_key, extent, split, smallest, largest):
    gain = 1.0
    for axis_at, blocks in split:
        steps = jax.random.uniform(jax.random.fold_in(jax.random.fold_in(stream_key, 6), axis_at), (blocks,), jnp.float32, smallest / len(split), largest / len(split))
        gain = gain * jnp.repeat(jnp.exp(steps), extent[axis_at] // blocks).reshape((-1,) + (1,) * (len(extent) - 1 - axis_at))
    return gain


def rank_table(number_of, lean):
    weights = [(1 << 20) // math.isqrt(grade ** lean) + 1 for grade in range(1, number_of + 1)]
    deviation = 1 + sum(weights) // (1 << 30)
    return np.cumsum(np.array([max(1, weight // deviation) for weight in weights]))


def ranked(rng, shape, count, skew):
    grid = rank_table(count, skew)
    ticket = jax.random.randint(jax.random.fold_in(rng, 1), shape, 0, int(grid[count - 1]))
    grade = jnp.searchsorted(jnp.asarray(grid, jnp.int32), ticket, side="right")
    return jax.random.permutation(jax.random.fold_in(rng, 2), count)[grade].astype(jnp.int32)


def normal_values(key, shape, scale, bound, split=(), kind=jnp.bfloat16):
    entries = scale * jax.random.normal(key, shape, jnp.float32)
    if split:
        entries = entries * block_levels(key, shape, split, -0.22, 0.18)
    return jnp.clip(entries, -bound, bound).astype(kind)


def heavy_noise(key, shape, deviation, reach, pieces, heavy, kind=jnp.bfloat16):
    array = deviation * jax.random.normal(key, shape, jnp.float32)
    if pieces:
        array = array * block_levels(key, shape, pieces, -0.22, 0.18)
    return jnp.clip(spiked(array, jax.random.fold_in(key, 3), *heavy), -reach, reach).astype(kind)


def setup_inputs(seed: int = 0) -> dict:
    seeds = jax.random.split(jax.random.key(seed), 5)
    amplitudes = normal_values(seeds[0], (PAIRS, NT * TILE), 1.0, 6.0, ((0, 4), (1, 64)))
    integrals = heavy_noise(seeds[1], (NT * TILE, NT * TILE), (NT * TILE // NSYM) ** -0.5, 0.25, ((0, 64), (1, 4)), (0, 1, 64, 4.0))
    labels = touch_ends(ranked(seeds[2], (NT,), NSYM, 2), jax.random.fold_in(seeds[2], 3), 0, NSYM - 1).astype(jnp.int32)
    slot_tile = jax.random.permutation(seeds[3], NT).astype(jnp.int32)
    return dict(amplitudes=amplitudes, integrals=integrals, labels=labels, slot_tile=slot_tile)


def reference(amplitudes, integrals, labels, slot_tile):
    slot_label = labels[slot_tile]
    row_label = jnp.repeat(slot_label, TILE)

    def one_tile(index):
        columns = lax.dynamic_slice_in_dim(integrals, index * TILE, TILE, 1)
        keep = (row_label == labels[index]).astype(jnp.bfloat16)
        masked = columns * keep[:, None]
        return jnp.dot(amplitudes, masked, preferred_element_type=jnp.float32)

    blocks = lax.map(one_tile, jnp.arange(NT, dtype=jnp.int32))
    return jnp.transpose(blocks, (1, 0, 2)).reshape(amplitudes.shape[0], NT * TILE)
```

```python
import functools

import jax
import jax.numpy as jnp
from jax import lax
from jax.experimental import pallas as pl
from jax.experimental.pallas import tpu as pltpu
from jax.sharding import Mesh
from jax.sharding import PartitionSpec as P

TILE = 128
VIR = ("vir_0", "vir_1", "vir_2", "vir_3")
OCC_VIR = ("occ", "vir_0", "vir_1", "vir_2", "vir_3")
MESH = pl.DeviceIdType.MESH
CHUNKS = 4
LOG_STEP = 350.0
TOP = 32700.0


def coded(value):
    rows = value.shape[0]
    parts = value.reshape(rows // 8, 8, TILE)
    largest = jnp.maximum(jnp.max(jnp.abs(parts), axis=0), 1e-30)
    level = jnp.ceil(jnp.log(largest) * LOG_STEP)
    scaled = parts * (jnp.exp(level * (-1.0 / LOG_STEP)) * TOP)[None]
    scaled = jnp.round(scaled).reshape(rows, TILE)
    pad = [level] if rows % 16 else [level, level]
    return jnp.concatenate([scaled, *pad], axis=0).astype(jnp.int32).astype(jnp.int16)


def decoded(message, rows):
    value = message.astype(jnp.int32).astype(jnp.float32)
    scale = jnp.exp(value[rows : rows + 8] * (1.0 / LOG_STEP)) * (1.0 / TOP)
    parts = value[:rows].reshape(rows // 8, 8, TILE) * scale[None]
    return parts.reshape(rows, TILE)


def kernel(
    rows,
    amp_ref, int_ref, labels_ref, slot_ref, out_ref,
    amp, own, other, acc, plane, tower, s1, r1, s2, r2, s3, r3,
    own_sem, swap_send, swap_recv, amp_sem, mate_send, mate_recv, occ_send, occ_recv,
    s1_sem, r1_sem, s2_sem, r2_sem, s3_sem, r3_sem,
):
    occ = lax.axis_index("occ")
    y, x, zh, core = (lax.axis_index(name) for name in VIR)
    vir = ((y * 4 + x) * 2 + zh) * 2 + core
    mate = 1 - core
    blocks = [occ, occ + 1 - 2 * lax.rem(occ, 2), lax.rem(occ + 2, 4), 3 - occ]
    place = {"vir_0": y, "vir_1": x}
    up = {axis: lax.rem(at + 1, 4) for axis, at in place.items()}
    down = {axis: lax.rem(at + 3, 4) for axis, at in place.items()}
    far = {axis: lax.rem(at + 2, 4) for axis, at in place.items()}

    def copy_to(src, dst, send, recv, device):
        return pltpu.make_async_remote_copy(
            src_ref=src, dst_ref=dst, send_sem=send, recv_sem=recv,
            device_id=device, device_id_type=MESH,
        )

    def columns(pair, half, parity):
        tile = (pair * 2 + half) * 2 + parity
        return int_ref.at[:, pl.ds(pl.multiple_of(tile * TILE, TILE), TILE)]

    for pair in range(16):
        for half in range(2):
            pltpu.make_async_copy(
                columns(pair, half, core),
                own.at[pair, :, pl.ds(half * TILE, TILE)],
                own_sem.at[pair // 4],
            ).start()
    own_amp = pltpu.make_async_copy(amp_ref, amp.at[occ, core], amp_sem)
    own_amp.start()

    barrier = pltpu.get_barrier_semaphore()
    partners = [{"vir_3": mate}, {"vir_2": 1 - zh}]
    for axis in place:
        partners += [{axis: up[axis]}, {axis: down[axis]}]
    partners += [{"occ": block} for block in blocks[1:]]
    for partner in partners:
        pl.semaphore_signal(barrier, inc=1, device_id=partner, device_id_type=MESH)
    pl.semaphore_wait(barrier, len(partners))

    sent = []

    def send(*args):
        copy = copy_to(*args)
        copy.start()
        sent.append(copy)

    send(amp_ref, amp.at[occ, core], mate_send.at[0], mate_recv.at[occ], {"vir_3": mate})
    for step in range(1, CHUNKS):
        send(
            amp_ref, amp.at[occ, core], occ_send.at[step], occ_recv.at[occ],
            {"occ": blocks[step]},
        )
    for pair in range(16):
        for half in range(2):
            copy_to(
                columns(pair, half, mate),
                other.at[pair, :, pl.ds(half * TILE, TILE)],
                swap_send.at[pair // 4], swap_recv.at[pair // 4], {"vir_3": mate},
            ).start()

    def group_wait(buffer, group, sem):
        part = buffer.at[pl.ds(group * 4, 4)]
        pltpu.make_async_copy(part, part, sem.at[group]).wait()

    def forward(step):
        block = blocks[step]
        here = amp.at[block, core]
        copy_to(here, here, occ_send.at[step], occ_recv.at[block], {"occ": block}).wait_recv()
        send(here, here, mate_send.at[step], mate_recv.at[block], {"vir_3": mate})

    lane = lax.broadcasted_iota(jnp.int32, (1, 2 * TILE), 1)
    own_first = vir * 4
    other_first = (vir + 1 - 2 * core) * 4

    def keep(first, pair, slot):
        label = labels_ref[slot_ref[first + slot]]
        tile = occ * 64 + pair * 4 + core
        low = jnp.where(label == labels_ref[tile], 1.0, 0.0)
        high = jnp.where(label == labels_ref[tile + 2], 1.0, 0.0)
        return jnp.where(lane < TILE, low, high).astype(jnp.bfloat16)

    def compute(step):
        block = blocks[step]
        if step == 0:
            own_amp.wait()
        there = amp.at[block, mate]
        copy_to(there, there, mate_send.at[step], mate_recv.at[block], {"vir_3": mate}).wait_recv()

        for group in range(4):
            if step == 0:
                group_wait(own, group, own_sem)
                group_wait(other, group, swap_recv)

            def one(pair, _):
                pair = pair + group * 4
                if step == 0:
                    for buffer, first in ((own, own_first), (other, other_first)):
                        for slot in range(4):
                            at = pl.ds(slot * TILE, TILE)
                            buffer[pair, at, :] = buffer[pair, at, :] * keep(first, pair, slot)
                acc[step, pair] = jnp.dot(
                    amp[block, core], own[pair], preferred_element_type=jnp.float32
                ) + jnp.dot(
                    amp[block, mate], other[pair], preferred_element_type=jnp.float32
                )
                return 0

            lax.fori_loop(0, 4, one, 0, unroll=True)

    FIRST = ("vir_1", "vir_0")
    SECOND = ("vir_0", "vir_1")

    def two_tiles(step, colour, target, part):
        found = []
        for other_at in (2 * part, 2 * part + 1):
            pair = other_at * 4 + target if colour == 0 else target * 4 + other_at
            found.append(acc[step, pair, :, pl.ds(colour * TILE, TILE)])
        return jnp.concatenate(found, axis=0)

    def send1(step, colour, way, kind, value):
        axis = FIRST[colour]
        at = (step, colour, way, kind)
        s1[at] = coded(value)
        send(
            s1.at[at], r1.at[at], s1_sem.at[at], r1_sem.at[at],
            {axis: (up, down)[way][axis]},
        )

    def take1(step, colour, way, kind):
        at = (step, colour, way, kind)
        axis = FIRST[colour]
        copy_to(
            s1.at[at], r1.at[at], s1_sem.at[at], r1_sem.at[at], {axis: up[axis]}
        ).wait_recv()
        return decoded(r1[at], 2 * rows)

    def first_send(step):
        for colour in range(2):
            axis = FIRST[colour]
            for way in range(2):
                send1(step, colour, way, 0, two_tiles(step, colour, far[axis], way))
        for colour in range(2):
            axis = FIRST[colour]
            for way in range(2):
                near = (up, down)[way][axis]
                send1(step, colour, way, 1, two_tiles(step, colour, near, 1 - way))

    def first_relay(step):
        for colour in range(2):
            axis = FIRST[colour]
            for way in range(2):
                near = (up, down)[way][axis]
                send1(
                    step, colour, way, 2,
                    take1(step, colour, way, 0) + two_tiles(step, colour, near, way),
                )

    def send2(step, colour, way, kind, value):
        axis = SECOND[colour]
        at = (step, colour, kind)
        s2[at] = coded(value)
        send(
            s2.at[at], r2.at[at], s2_sem.at[at], r2_sem.at[at],
            {axis: (up, down)[way][axis]},
        )

    def take2(step, colour, kind):
        at = (step, colour, kind)
        axis = SECOND[colour]
        copy_to(
            s2.at[at], r2.at[at], s2_sem.at[at], r2_sem.at[at], {axis: up[axis]}
        ).wait_recv()
        return decoded(r2[at], rows)

    def first_end(step):
        for colour in range(2):
            axis = FIRST[colour]
            for part in range(2):
                total = (
                    two_tiles(step, colour, place[axis], part)
                    + take1(step, colour, 1 - part, 1)
                    + take1(step, colour, part, 2)
                )
                plane[step, colour, 2 * part] = total[:rows]
                plane[step, colour, 2 * part + 1] = total[rows:]
            way = step % 2
            axis = SECOND[colour]
            send2(step, colour, way, 0, plane[step, colour, far[axis]])
            back = (down, up)[way][axis]
            send2(step, colour, 1 - way, 1, plane[step, colour, back])

    def second_relay(step):
        way = step % 2
        for colour in range(2):
            near = (up, down)[way][SECOND[colour]]
            send2(
                step, colour, way, 2,
                take2(step, colour, 0) + plane[step, colour, near],
            )

    def second_end(step):
        for colour in range(2):
            here = place[SECOND[colour]]
            tower[step, colour] = (
                plane[step, colour, here] + take2(step, colour, 1) + take2(step, colour, 2)
            )
        s3[step] = coded(tower[step, 1 - zh])
        send(s3.at[step], r3.at[step], s3_sem.at[step], r3_sem.at[step], {"vir_2": 1 - zh})

    def finish(step):
        copy_to(
            s3.at[step], r3.at[step], s3_sem.at[step], r3_sem.at[step], {"vir_2": 1 - zh}
        ).wait_recv()
        at = pl.ds(pl.multiple_of(blocks[step] * rows, 8), rows)
        out_ref[at, :] = tower[step, zh] + decoded(r3[step], rows)

    stages = (compute, first_send, first_relay, first_end, second_relay, second_end, finish)
    for tick in range(CHUNKS + 5):
        for step in range(CHUNKS - 1, -1, -1):
            age = tick - step
            if age == 0:
                if step + 1 < CHUNKS:
                    forward(step + 1)
                compute(step)
                first_send(step)
            elif 0 < age < 6:
                stages[age + 1](step)

    for copy in sent:
        copy.wait_send()
    for group in range(4):
        group_wait(own, group, swap_send)


def shards(amplitudes, integrals, labels, slot_tile):
    rows = amplitudes.shape[0]
    depth = integrals.shape[0]
    vmem = pltpu.VMEM
    dma = pltpu.SemaphoreType.DMA
    first = (CHUNKS, 2, 2, 3)
    second = (CHUNKS, 2, 3)
    return pl.pallas_call(
        functools.partial(kernel, rows),
        out_shape=jax.ShapeDtypeStruct((CHUNKS * rows, TILE), jnp.float32),
        in_specs=[
            pl.BlockSpec(memory_space=pl.ANY),
            pl.BlockSpec(memory_space=pl.ANY),
            pl.BlockSpec(memory_space=pltpu.SMEM),
            pl.BlockSpec(memory_space=pltpu.SMEM),
        ],
        out_specs=pl.BlockSpec(memory_space=vmem),
        scratch_shapes=[
            vmem((CHUNKS, 2, rows, depth), jnp.bfloat16),
            vmem((16, depth, 2 * TILE), jnp.bfloat16),
            vmem((16, depth, 2 * TILE), jnp.bfloat16),
            vmem((CHUNKS, 16, rows, 2 * TILE), jnp.float32),
            vmem((CHUNKS, 2, 4, rows, TILE), jnp.float32),
            vmem((CHUNKS, 2, rows, TILE), jnp.float32),
            vmem((*first, 2 * rows + 16, TILE), jnp.int16),
            vmem((*first, 2 * rows + 16, TILE), jnp.int16),
            vmem((*second, rows + 8, TILE), jnp.int16),
            vmem((*second, rows + 8, TILE), jnp.int16),
            vmem((CHUNKS, rows + 8, TILE), jnp.int16),
            vmem((CHUNKS, rows + 8, TILE), jnp.int16),
            dma((4,)), dma((4,)), dma((4,)), dma,
            dma((CHUNKS,)), dma((CHUNKS,)), dma((CHUNKS,)), dma((CHUNKS,)),
            dma(first), dma(first), dma(second), dma(second), dma((CHUNKS,)), dma((CHUNKS,)),
        ],
        compiler_params=pltpu.CompilerParams(
            collective_id=0, has_side_effects=True, vmem_limit_bytes=48 * 1024 * 1024
        ),
        name="ladder",
    )(amplitudes, integrals, labels, slot_tile)


def solution(mesh):
    split = Mesh(
        mesh.devices.reshape(mesh.shape["occ"], 4, 4, 2, 2),
        ("occ", "vir_0", "vir_1", "vir_2", "vir_3"),
    )
    placed = (P("occ", VIR), P(VIR, "occ"), P(), P())
    return jax.shard_map(
        shards, mesh=split, in_specs=placed, out_specs=P(None, OCC_VIR), check_vma=False
    )
```

```python
import functools

import jax
import jax.numpy as jnp
from jax import lax
from jax.experimental import pallas as pl
from jax.experimental.pallas import tpu as pltpu
from jax.sharding import Mesh
from jax.sharding import PartitionSpec as P

TILE = 128
VIR = ("vir_0", "vir_1", "vir_2", "vir_3")
OCC_VIR = ("occ", "vir_0", "vir_1", "vir_2", "vir_3")
MESH = pl.DeviceIdType.MESH
CHUNKS = 4
LOG_STEP = 350.0
TOP = 32700.0


def coded(value):
    rows = value.shape[0]
    parts = value.reshape(rows // 8, 8, TILE)
    largest = jnp.maximum(jnp.max(jnp.abs(parts), axis=0), 1e-30)
    level = jnp.ceil(jnp.log(largest) * LOG_STEP)
    scaled = parts * (jnp.exp(level * (-1.0 / LOG_STEP)) * TOP)[None]
    scaled = jnp.round(scaled).reshape(rows, TILE)
    pad = [level] if rows % 16 else [level, level]
    return jnp.concatenate([scaled, *pad], axis=0).astype(jnp.int32).astype(jnp.int16)


def decoded(message, rows):
    value = message.astype(jnp.int32).astype(jnp.float32)
    scale = jnp.exp(value[rows : rows + 8] * (1.0 / LOG_STEP)) * (1.0 / TOP)
    parts = value[:rows].reshape(rows // 8, 8, TILE) * scale[None]
    return parts.reshape(rows, TILE)


def kernel(
    rows, parts, order, direct,
    amp_ref, int_ref, labels_ref, slot_ref, out_ref,
    labels, slots, amp, integ, acc, macc, plane, tower, s1, r1, s2, r2, s3, r3,
    small_sem, int_sem, ready_sem, occ_send, occ_recv, mate_send, mate_recv,
    s1_sem, r1_sem, s2_sem, r2_sem, s3_sem, r3_sem,
):
    occ = lax.axis_index("occ")
    y, x, zh, core = (lax.axis_index(name) for name in VIR)
    vir = ((y * 4 + x) * 2 + zh) * 2 + core
    mate = 1 - core
    inner = jnp.logical_and(occ > 0, occ < 3)
    two_on, opposite = lax.rem(occ + 2, 4), 3 - occ
    blocks = [
        occ, occ + 1 - 2 * lax.rem(occ, 2),
        jnp.where(inner, opposite, two_on), jnp.where(inner, two_on, opposite),
    ]
    place = {"vir_0": y, "vir_1": x}
    up = {axis: lax.rem(at + 1, 4) for axis, at in place.items()}
    down = {axis: lax.rem(at + 3, 4) for axis, at in place.items()}
    far = {axis: lax.rem(at + 2, 4) for axis, at in place.items()}
    FIRST = ("vir_1", "vir_0")
    SECOND = ("vir_0", "vir_1")

    def copy_to(src, dst, send, recv, device):
        return pltpu.make_async_remote_copy(
            src_ref=src, dst_ref=dst, send_sem=send, recv_sem=recv,
            device_id=device, device_id_type=MESH,
        )

    def pair_of(colour, dest, j):
        return j * 4 + dest if colour == 0 else dest * 4 + j

    def wait_for(part, sem):
        pltpu.make_async_copy(part, part, sem).wait()

    small = [
        pltpu.make_async_copy(labels_ref, labels, small_sem.at[0]),
        pltpu.make_async_copy(slot_ref, slots, small_sem.at[1]),
        pltpu.make_async_copy(amp_ref, amp.at[occ], small_sem.at[2]),
    ]
    for copy in small:
        copy.start()
    def fetch(turn, _):
        steps = jnp.where(turn < 2, 2 - turn, 3 * (3 - turn))
        for colour in range(2):
            dest = lax.rem(place[FIRST[colour]] + steps, 4)
            for j in range(4):
                first = (pair_of(colour, dest, j) * 2 + colour) * 2 * TILE
                pltpu.make_async_copy(
                    int_ref.at[:, pl.ds(pl.multiple_of(first, 2 * TILE), 2 * TILE)],
                    integ.at[colour, dest, j],
                    int_sem.at[colour, dest],
                ).start()
        return 0

    lax.fori_loop(0, 4, fetch, 0)

    barrier = pltpu.get_barrier_semaphore()
    partners = [{"vir_3": mate}]
    for axis in place:
        partners += [{axis: up[axis]}, {axis: down[axis]}, {axis: far[axis]}]
    partners += [{"occ": block} for block in blocks[1:]]
    for partner in partners:
        pl.semaphore_signal(barrier, inc=1, device_id=partner, device_id_type=MESH)

    @pl.when(zh == 0)
    def _():
        pl.semaphore_signal(barrier, inc=1, device_id={"vir_2": 1 - zh}, device_id_type=MESH)

    def send(*args):
        copy_to(*args).start()

    def keep(colour, dest, j, slot):
        label = labels[slots[vir * 4 + slot]]
        tile = occ * 64 + (pair_of(colour, dest, j) * 2 + colour) * 2
        lane = lax.broadcasted_iota(jnp.int32, (1, 2 * TILE), 1)
        low = jnp.where(label == labels[tile], 1.0, 0.0)
        high = jnp.where(label == labels[tile + 1], 1.0, 0.0)
        return jnp.where(lane < TILE, low, high).astype(jnp.bfloat16)

    def multiply(step, colour, dest):
        if step == 0:
            wait_for(integ.at[colour, dest], int_sem.at[colour, dest])
        for j in range(4):
            if step == 0:
                for slot in range(4):
                    at = pl.ds(slot * TILE, TILE)
                    integ[colour, dest, j, at, :] = (
                        integ[colour, dest, j, at, :] * keep(colour, dest, j, slot)
                    )
            found = jnp.dot(
                amp[blocks[step]], integ[colour, dest, j], preferred_element_type=jnp.float32
            )
            for parity in range(2):
                acc[step, parity, colour, dest, j] = found[:, parity * TILE : (parity + 1) * TILE]

    groups = {id(far): (0, 1), id(up): (2, 2), id(down): (2, 2), id(place): (3, 3)}

    def units(step, where):
        for colour in range(2):
            multiply(step, colour, where[FIRST[colour]])

    def hand_over(step, where):
        for colour in range(2):
            dest = where[FIRST[colour]]
            send(
                acc.at[step, mate, colour, dest], macc.at[step, colour, dest],
                mate_send.at[step], mate_recv.at[step, groups[id(where)][colour]],
                {"vir_3": mate},
            )

    taken = set()

    def take_over(chunk, group):
        step = parts[chunk][0]
        if (step, group) not in taken:
            taken.add((step, group))
            part = (
                macc.at[step, 0, 0], macc.at[step, 0, 0],
                macc.at[step, 0], macc.at[step, 0, pl.ds(0, 2)],
            )[group]
            wait_for(part, mate_recv.at[step, group])

    def to_peer(step):
        send(
            amp.at[occ], amp.at[occ], occ_send, occ_recv.at[occ], {"occ": blocks[step]}
        )

    def product(step):
        wait_for(amp.at[blocks[step]], occ_recv.at[blocks[step]])
        for where in (far, up, down, place):
            units(step, where)
            hand_over(step, where)

    def two_tiles(chunk, colour, target, part):
        step, start, count = parts[chunk]
        at = (colour, target, pl.ds(2 * part, 2), pl.ds(start, count))
        return (acc[(step, core, *at)] + macc[(step, *at)]).reshape(2 * count, TILE)

    def message(buffer, at, count):
        return buffer.at[(*at, pl.ds(0, count + 16 - count % 16))]

    def send1(chunk, colour, way, kind, value):
        axis = FIRST[colour]
        at = (chunk, colour, way, kind)
        out = message(s1, at, value.shape[0])
        out[...] = coded(value)
        send(
            out, message(r1, at, value.shape[0]),
            s1_sem.at[chunk], r1_sem.at[chunk, colour, min(kind, 1)],
            {axis: (up, down)[way][axis]},
        )

    def sizes(chunk):
        count = parts[chunk][2]
        return pl.ds(0, 2 * count + 16), pl.ds(0, count + 16 - count % 16)

    def take1(chunk, colour, way, kind):
        count = 2 * parts[chunk][2]
        return decoded(message(r1, (chunk, colour, way, kind), count)[...], count)

    def first_far(chunk):
        for colour in range(2):
            take_over(chunk, colour)
            for way in range(2):
                value = two_tiles(chunk, colour, far[FIRST[colour]], way)
                send1(chunk, colour, way, 0, value)

    def first_near(chunk):
        take_over(chunk, 2)
        for way in range(2):
            for colour in range(2):
                near = (up, down)[way]
                value = two_tiles(chunk, colour, near[FIRST[colour]], 1 - way)
                send1(chunk, colour, way, 1, value)

    def first_send(chunk):
        first_far(chunk)
        first_near(chunk)

    def first_relay(chunk):
        for colour in range(2):
            wait_for(r1.at[chunk, colour, :, 0, sizes(chunk)[0]], r1_sem.at[chunk, colour, 0])
            for way in range(2):
                near = (up, down)[way][FIRST[colour]]
                value = two_tiles(chunk, colour, near, way)
                send1(chunk, colour, way, 2, take1(chunk, colour, way, 0) + value)

    def send2(chunk, colour, kind, value, target):
        at = (chunk, colour, kind)
        out = message(s2, at, value.shape[0])
        out[...] = coded(value)
        send(
            out, message(r2, at, value.shape[0]),
            s2_sem.at[chunk], r2_sem.at[chunk, min(kind, 1)],
            {SECOND[colour]: target[SECOND[colour]]},
        )

    def take2(chunk, colour, kind):
        count = parts[chunk][2]
        return decoded(message(r2, (chunk, colour, kind), count)[...], count)

    def arrive2(chunk, group):
        kinds = pl.ds(0, 1) if group == 0 else pl.ds(1, 2)
        wait_for(r2.at[chunk, :, kinds, sizes(chunk)[1]], r2_sem.at[chunk, group])

    def ways(chunk):
        return (up, down) if chunk % 2 == 0 else (down, up)

    def first_end(chunk):
        onward, back = ways(chunk)
        step, start, count = parts[chunk]
        at = pl.ds(start, count)
        for colour in range(2):
            axis = FIRST[colour]
            take_over(chunk, 3)
            wait_for(
                r1.at[chunk, colour, :, pl.ds(1, 2), sizes(chunk)[0]],
                r1_sem.at[chunk, colour, 1],
            )
            for part in range(2):
                total = (
                    two_tiles(chunk, colour, place[axis], part)
                    + take1(chunk, colour, 1 - part, 1)
                    + take1(chunk, colour, part, 2)
                )
                plane[step, colour, 2 * part, at] = total[:count]
                plane[step, colour, 2 * part + 1, at] = total[count:]
            axis = SECOND[colour]
            to_far = far if chunk in direct else onward
            send2(chunk, colour, 0, plane[step, colour, far[axis], at], to_far)
            send2(chunk, colour, 1, plane[step, colour, back[axis], at], back)
            if chunk in direct:
                send2(chunk, colour, 2, plane[step, colour, onward[axis], at], onward)

    def second_relay(chunk):
        if chunk in direct:
            return
        onward, _ = ways(chunk)
        step, start, count = parts[chunk]
        arrive2(chunk, 0)
        for colour in range(2):
            value = plane[step, colour, onward[SECOND[colour]], pl.ds(start, count)]
            send2(chunk, colour, 2, take2(chunk, colour, 0) + value, onward)

    def second_end(chunk):
        step, start, count = parts[chunk]
        at = pl.ds(start, count)
        if chunk in direct:
            arrive2(chunk, 0)
        arrive2(chunk, 1)
        for colour in range(2):
            total = plane[step, colour, place[SECOND[colour]], at]
            for kind in range(0 if chunk in direct else 1, 3):
                total = total + take2(chunk, colour, kind)
            tower[step, colour, at] = total
        out = message(s3, (chunk,), count)
        out[...] = coded(tower[step, 1 - zh, at])
        if chunk == 0:

            @pl.when(zh == 0)
            def _():
                pl.semaphore_wait(ready_sem, 1)

        send(
            out, message(r3, (chunk,), count), s3_sem.at[chunk], r3_sem.at[chunk],
            {"vir_2": 1 - zh},
        )

    def finish(chunk):
        step, start, count = parts[chunk]
        here = message(r3, (chunk,), count)
        wait_for(here, r3_sem.at[chunk])
        at = pl.ds(pl.multiple_of(blocks[step] * rows + start, 8), count)
        out_ref[at, :] = tower[step, zh, pl.ds(start, count)] + decoded(here[...], count)

    for copy in small:
        copy.wait()
    units(0, far)

    pl.semaphore_wait(barrier, len(partners) + zh)

    to_peer(1)

    @pl.when(zh == 1)
    def _():
        pl.semaphore_signal(ready_sem, inc=1, device_id={"vir_2": 1 - zh}, device_id_type=MESH)

    @pl.when(inner)
    def _():
        to_peer(2)
        to_peer(3)

    hand_over(0, far)
    units(0, up)
    hand_over(0, up)
    units(0, down)
    hand_over(0, down)
    first_far(0)
    units(0, place)
    hand_over(0, place)
    first_near(0)

    @pl.when(jnp.logical_not(inner))
    def _():
        to_peer(2)
        to_peer(3)


    stages = {
        "P": product, "S": first_send, "R": first_relay, "F": first_end,
        "G": second_relay, "H": second_end, "Z": finish,
    }
    for row in order:
        for kind, number in zip(row[::2], row[1::2]):
            stages[kind](int(number))

    wait_for(amp.at[pl.ds(0, CHUNKS - 1)], occ_send)
    for step in range(CHUNKS):
        wait_for(acc.at[step, mate], mate_send.at[step])
    for chunk in range(len(parts)):
        wait_for(s1.at[chunk, :, :, :, sizes(chunk)[0]], s1_sem.at[chunk])
        wait_for(s2.at[chunk, :, :, sizes(chunk)[1]], s2_sem.at[chunk])
        wait_for(s3.at[chunk, sizes(chunk)[1]], s3_sem.at[chunk])


PARTS = ((0, 0, 88), (1, 0, 88), (2, 0, 88), (3, 0, 48), (3, 48, 40))
DIRECT = (3, 4)
ORDER = (
    "P1R0S1P2F0R1S2P3G0F1R2S3S4H0G1F2R3R4H1",
    "G2F3F4H2H3H4Z0Z1Z2Z3Z4",
)


def shards(amplitudes, integrals, labels, slot_tile):
    rows = amplitudes.shape[0]
    depth = integrals.shape[0]
    vmem = pltpu.VMEM
    dma = pltpu.SemaphoreType.DMA
    third = (len(PARTS),)
    first = (*third, 2, 2, 3)
    second = (*third, 2, 3)
    return pl.pallas_call(
        functools.partial(kernel, rows, PARTS, ORDER, DIRECT),
        out_shape=vmem((CHUNKS * rows, TILE), jnp.float32),
        in_specs=[pl.BlockSpec(memory_space=pltpu.HBM)] * 4,
        out_specs=pl.BlockSpec(memory_space=vmem),
        scratch_shapes=[
            pltpu.SMEM(labels.shape, jnp.int32),
            pltpu.SMEM(slot_tile.shape, jnp.int32),
            vmem((CHUNKS, rows, depth), jnp.bfloat16),
            vmem((2, 4, 4, depth, 2 * TILE), jnp.bfloat16),
            vmem((CHUNKS, 2, 2, 4, 4, rows, TILE), jnp.float32),
            vmem((CHUNKS, 2, 4, 4, rows, TILE), jnp.float32),
            vmem((CHUNKS, 2, 4, rows, TILE), jnp.float32),
            vmem((CHUNKS, 2, rows, TILE), jnp.float32),
            vmem((*first, 2 * rows + 16, TILE), jnp.int16),
            vmem((*first, 2 * rows + 16, TILE), jnp.int16),
            vmem((*second, rows + 8, TILE), jnp.int16),
            vmem((*second, rows + 8, TILE), jnp.int16),
            vmem((*third, rows + 8, TILE), jnp.int16),
            vmem((*third, rows + 8, TILE), jnp.int16),
            dma((3,)), dma((2, 4)), pltpu.SemaphoreType.REGULAR, dma, dma((CHUNKS,)), dma((CHUNKS,)), dma((CHUNKS, 4)),
            dma(third), dma((*third, 2, 2)), dma(third), dma((*third, 2)), dma(third), dma(third),
        ],
        compiler_params=pltpu.CompilerParams(
            collective_id=0, has_side_effects=True, vmem_limit_bytes=60 * 1024 * 1024
        ),
        name="ladder",
    )(amplitudes, integrals, labels, slot_tile)


def solution(mesh):
    split = Mesh(
        mesh.devices.reshape(mesh.shape["occ"], 4, 4, 2, 2),
        ("occ", "vir_0", "vir_1", "vir_2", "vir_3"),
    )
    placed = (P("occ", VIR), P(VIR, "occ"), P(), P())
    return jax.shard_map(
        shards, mesh=split, in_specs=placed, out_specs=P(None, OCC_VIR), check_vma=False
    )
```

```python
import functools

import jax
import jax.numpy as jnp
from jax import lax
from jax.experimental import pallas as pl
from jax.experimental.pallas import tpu as pltpu
from jax.sharding import Mesh
from jax.sharding import PartitionSpec as P

TILE = 128
VIR = ("vir_0", "vir_1", "vir_2", "vir_3")
OCC_VIR = ("occ", "vir_0", "vir_1", "vir_2", "vir_3")
MESH = pl.DeviceIdType.MESH
CHUNKS = 4
LOG_STEP = 350.0
TOP = 32700.0


def coded(value):
    rows = value.shape[0]
    parts = value.reshape(rows // 8, 8, TILE)
    largest = jnp.maximum(jnp.max(jnp.abs(parts), axis=0), 1e-30)
    level = jnp.ceil(jnp.log(largest) * LOG_STEP)
    scaled = parts * (jnp.exp(level * (-1.0 / LOG_STEP)) * TOP)[None]
    scaled = jnp.round(scaled).reshape(rows, TILE)
    return jnp.concatenate([scaled, level], axis=0).astype(jnp.int32).astype(jnp.int16)


def decoded(message, rows):
    value = message.astype(jnp.int32).astype(jnp.float32)
    scale = jnp.exp(value[rows : rows + 8] * (1.0 / LOG_STEP)) * (1.0 / TOP)
    parts = value[:rows].reshape(rows // 8, 8, TILE) * scale[None]
    return parts.reshape(rows, TILE)


def kernel(
    rows, parts, order, direct,
    amp_ref, int_ref, labels_ref, slot_ref, out_ref,
    labels, slots, amp, integ, acc, macc, plane, tower, s1, r1, s2, r2, s3, r3,
    small_sem, int_sem, ready_sem, occ_send, occ_recv, mate_send, mate_recv,
    s1_sem, r1_sem, s2_sem, r2_sem, s3_sem, r3_sem,
):
    occ = lax.axis_index("occ")
    y, x, zh, core = (lax.axis_index(name) for name in VIR)
    vir = ((y * 4 + x) * 2 + zh) * 2 + core
    mate = 1 - core
    inner = jnp.logical_and(occ > 0, occ < 3)
    two_on, opposite = lax.rem(occ + 2, 4), 3 - occ
    blocks = [
        occ, occ + 1 - 2 * lax.rem(occ, 2),
        jnp.where(inner, opposite, two_on), jnp.where(inner, two_on, opposite),
    ]
    place = {"vir_0": y, "vir_1": x}
    up = {axis: lax.rem(at + 1, 4) for axis, at in place.items()}
    down = {axis: lax.rem(at + 3, 4) for axis, at in place.items()}
    far = {axis: lax.rem(at + 2, 4) for axis, at in place.items()}
    FIRST = ("vir_1", "vir_0")
    SECOND = ("vir_0", "vir_1")

    def copy_to(src, dst, send, recv, device):
        return pltpu.make_async_remote_copy(
            src_ref=src, dst_ref=dst, send_sem=send, recv_sem=recv,
            device_id=device, device_id_type=MESH,
        )

    def pair_of(colour, dest, j):
        return j * 4 + dest if colour == 0 else dest * 4 + j

    def wait_for(part, sem):
        pltpu.make_async_copy(part, part, sem).wait()

    small = [
        pltpu.make_async_copy(labels_ref, labels, small_sem.at[0]),
        pltpu.make_async_copy(slot_ref, slots, small_sem.at[1]),
        pltpu.make_async_copy(amp_ref, amp.at[occ], small_sem.at[2]),
    ]
    for copy in small:
        copy.start()
    def fetch(turn, _):
        steps = jnp.where(turn < 2, 2 - turn, 3 * (3 - turn))
        for colour in range(2):
            dest = lax.rem(place[FIRST[colour]] + steps, 4)
            for j in range(4):
                first = (pair_of(colour, dest, j) * 2 + colour) * 2 * TILE
                pltpu.make_async_copy(
                    int_ref.at[:, pl.ds(pl.multiple_of(first, 2 * TILE), 2 * TILE)],
                    integ.at[colour, dest, j],
                    int_sem.at[colour, dest],
                ).start()
        return 0

    lax.fori_loop(0, 4, fetch, 0)

    barrier = pltpu.get_barrier_semaphore()
    partners = [{"vir_3": mate}]
    for axis in place:
        partners += [{axis: up[axis]}, {axis: down[axis]}, {axis: far[axis]}]
    partners += [{"occ": block} for block in blocks[1:]]
    for partner in partners:
        pl.semaphore_signal(barrier, inc=1, device_id=partner, device_id_type=MESH)

    @pl.when(zh == 0)
    def _():
        pl.semaphore_signal(barrier, inc=1, device_id={"vir_2": 1 - zh}, device_id_type=MESH)

    def send(*args):
        copy_to(*args).start()

    def keep(colour, dest, j, slot):
        label = labels[slots[vir * 4 + slot]]
        tile = occ * 64 + (pair_of(colour, dest, j) * 2 + colour) * 2
        lane = lax.broadcasted_iota(jnp.int32, (1, 2 * TILE), 1)
        low = jnp.where(label == labels[tile], 1.0, 0.0)
        high = jnp.where(label == labels[tile + 1], 1.0, 0.0)
        return jnp.where(lane < TILE, low, high).astype(jnp.bfloat16)

    def multiply(step, colour, dest):
        if step == 0:
            wait_for(integ.at[colour, dest], int_sem.at[colour, dest])
        for j in range(4):
            if step == 0:
                for slot in range(4):
                    at = pl.ds(slot * TILE, TILE)
                    integ[colour, dest, j, at, :] = (
                        integ[colour, dest, j, at, :] * keep(colour, dest, j, slot)
                    )
            found = jnp.dot(
                amp[blocks[step]], integ[colour, dest, j], preferred_element_type=jnp.float32
            )
            for parity in range(2):
                acc[step, parity, colour, dest, j] = found[:, parity * TILE : (parity + 1) * TILE]

    groups = {id(far): (0, 1), id(up): (2, 2), id(down): (2, 2), id(place): (3, 3)}

    def units(step, where):
        for colour in range(2):
            multiply(step, colour, where[FIRST[colour]])

    def hand_over(step, where):
        for colour in range(2):
            dest = where[FIRST[colour]]
            send(
                acc.at[step, mate, colour, dest], macc.at[step, colour, dest],
                mate_send.at[step], mate_recv.at[step, groups[id(where)][colour]],
                {"vir_3": mate},
            )

    taken = set()

    def take_over(chunk, group):
        step = parts[chunk][0]
        if (step, group) not in taken:
            taken.add((step, group))
            part = (
                macc.at[step, 0, 0], macc.at[step, 0, 0],
                macc.at[step, 0], macc.at[step, 0, pl.ds(0, 2)],
            )[group]
            wait_for(part, mate_recv.at[step, group])

    def to_peer(step):
        send(
            amp.at[occ], amp.at[occ], occ_send, occ_recv.at[occ], {"occ": blocks[step]}
        )

    def product(step):
        wait_for(amp.at[blocks[step]], occ_recv.at[blocks[step]])
        for where in (far, up, down, place):
            units(step, where)
            hand_over(step, where)

    def two_tiles(chunk, colour, target, part):
        step, start, count = parts[chunk]
        at = (colour, target, pl.ds(2 * part, 2), pl.ds(start, count))
        return (acc[(step, core, *at)] + macc[(step, *at)]).reshape(2 * count, TILE)

    def message(buffer, at, count):
        return buffer.at[(*at, pl.ds(0, count + 8))]

    def send1(chunk, colour, way, kind, value):
        axis = FIRST[colour]
        at = (chunk, colour, way, kind)
        out = message(s1, at, value.shape[0])
        out[...] = coded(value)
        send(
            out, message(r1, at, value.shape[0]),
            s1_sem.at[chunk], r1_sem.at[chunk, colour, min(kind, 1)],
            {axis: (up, down)[way][axis]},
        )

    def sizes(chunk):
        count = parts[chunk][2]
        return pl.ds(0, 2 * count + 8), pl.ds(0, count + 8)

    def take1(chunk, colour, way, kind):
        count = 2 * parts[chunk][2]
        return decoded(message(r1, (chunk, colour, way, kind), count)[...], count)

    def first_far(chunk, colour):
        take_over(chunk, colour)
        for way in range(2):
            value = two_tiles(chunk, colour, far[FIRST[colour]], way)
            send1(chunk, colour, way, 0, value)

    def first_near(chunk, colour):
        take_over(chunk, 2)
        for way in range(2):
            near = (up, down)[way]
            value = two_tiles(chunk, colour, near[FIRST[colour]], 1 - way)
            send1(chunk, colour, way, 1, value)

    def first_send(chunk, colour):
        first_far(chunk, colour)
        first_near(chunk, colour)

    def first_relay(chunk, colour):
        wait_for(r1.at[chunk, colour, :, 0, sizes(chunk)[0]], r1_sem.at[chunk, colour, 0])
        for way in range(2):
            near = (up, down)[way][FIRST[colour]]
            value = two_tiles(chunk, colour, near, way)
            send1(chunk, colour, way, 2, take1(chunk, colour, way, 0) + value)

    def send2(chunk, colour, kind, value, target):
        at = (chunk, colour, kind)
        out = message(s2, at, value.shape[0])
        out[...] = coded(value)
        send(
            out, message(r2, at, value.shape[0]),
            s2_sem.at[chunk], r2_sem.at[chunk, colour, min(kind, 1)],
            {SECOND[colour]: target[SECOND[colour]]},
        )

    def take2(chunk, colour, kind):
        count = parts[chunk][2]
        return decoded(message(r2, (chunk, colour, kind), count)[...], count)

    def arrive2(chunk, colour, group):
        kinds = pl.ds(0, 1) if group == 0 else pl.ds(1, 2)
        wait_for(r2.at[chunk, colour, kinds, sizes(chunk)[1]], r2_sem.at[chunk, colour, group])

    def ways(chunk):
        return (up, down) if chunk % 2 == 0 else (down, up)

    def first_end(chunk, colour):
        onward, back = ways(chunk)
        step, start, count = parts[chunk]
        at = pl.ds(start, count)
        axis = FIRST[colour]
        take_over(chunk, 3)
        wait_for(
            r1.at[chunk, colour, :, pl.ds(1, 2), sizes(chunk)[0]], r1_sem.at[chunk, colour, 1]
        )
        for part in range(2):
            total = (
                two_tiles(chunk, colour, place[axis], part)
                + take1(chunk, colour, 1 - part, 1)
                + take1(chunk, colour, part, 2)
            )
            plane[step, colour, 2 * part, at] = total[:count]
            plane[step, colour, 2 * part + 1, at] = total[count:]
        axis = SECOND[colour]
        to_far = far if chunk in direct else onward
        send2(chunk, colour, 0, plane[step, colour, far[axis], at], to_far)
        send2(chunk, colour, 1, plane[step, colour, back[axis], at], back)
        if chunk in direct:
            send2(chunk, colour, 2, plane[step, colour, onward[axis], at], onward)

    def second_relay(chunk, colour):
        if chunk in direct:
            return
        onward, _ = ways(chunk)
        step, start, count = parts[chunk]
        arrive2(chunk, colour, 0)
        value = plane[step, colour, onward[SECOND[colour]], pl.ds(start, count)]
        send2(chunk, colour, 2, take2(chunk, colour, 0) + value, onward)

    def second_end(chunk, colour):
        step, start, count = parts[chunk]
        at = pl.ds(start, count)
        if chunk in direct:
            arrive2(chunk, colour, 0)
        arrive2(chunk, colour, 1)
        total = plane[step, colour, place[SECOND[colour]], at]
        for kind in range(0 if chunk in direct else 1, 3):
            total = total + take2(chunk, colour, kind)
        tower[step, colour, at] = total

        @pl.when(zh == 1 - colour)
        def _():
            out = message(s3, (chunk,), count)
            out[...] = coded(total)
            if chunk == 0 and colour == 1:
                pl.semaphore_wait(ready_sem, 1)
            send(
                out, message(r3, (chunk,), count), s3_sem.at[chunk], r3_sem.at[chunk],
                {"vir_2": 1 - zh},
            )

    def finish(chunk):
        step, start, count = parts[chunk]
        here = message(r3, (chunk,), count)
        wait_for(here, r3_sem.at[chunk])
        at = pl.ds(pl.multiple_of(blocks[step] * rows + start, 8), count)
        out_ref[at, :] = tower[step, zh, pl.ds(start, count)] + decoded(here[...], count)

    for copy in small:
        copy.wait()
    units(0, far)

    pl.semaphore_wait(barrier, len(partners) + zh)

    to_peer(1)

    @pl.when(zh == 1)
    def _():
        pl.semaphore_signal(ready_sem, inc=1, device_id={"vir_2": 1 - zh}, device_id_type=MESH)

    @pl.when(inner)
    def _():
        to_peer(2)
        to_peer(3)

    hand_over(0, far)
    units(0, up)
    hand_over(0, up)
    units(0, down)
    hand_over(0, down)
    for colour in range(2):
        first_far(0, colour)
    units(0, place)
    hand_over(0, place)
    for colour in range(2):
        first_near(0, colour)

    @pl.when(jnp.logical_not(inner))
    def _():
        to_peer(2)
        to_peer(3)


    stages = {
        "s": first_send, "r": first_relay, "f": first_end, "g": second_relay, "h": second_end
    }
    for row in order:
        for kind, number in zip(row[::2], row[1::2]):
            if kind == "P":
                product(int(number))
            elif kind == "Z":
                finish(int(number))
            else:
                stages[kind.lower()](int(number), int(kind.isupper()))

    wait_for(amp.at[pl.ds(0, CHUNKS - 1)], occ_send)
    for step in range(CHUNKS):
        wait_for(acc.at[step, mate], mate_send.at[step])
    for chunk in range(len(parts)):
        wait_for(s1.at[chunk, :, :, :, sizes(chunk)[0]], s1_sem.at[chunk])
        wait_for(s2.at[chunk, :, :, sizes(chunk)[1]], s2_sem.at[chunk])
        wait_for(s3.at[chunk, sizes(chunk)[1]], s3_sem.at[chunk])


PARTS = ((0, 0, 88), (1, 0, 88), (2, 0, 88), (3, 0, 48), (3, 48, 40))
DIRECT = (3, 4)
ORDER = (
    "P1r0R0s1S1P2f0r1s2R1S2P3g0f1r2s3s4F0R2S3S4",
    "h0g1f2r3r4G0F1R3R4h1g2f3f4H0G1F2h2F3h3F4h4",
    "H1G2H2H3H4Z0Z1Z2Z3Z4",
)


def shards(amplitudes, integrals, labels, slot_tile):
    rows = amplitudes.shape[0]
    depth = integrals.shape[0]
    vmem = pltpu.VMEM
    dma = pltpu.SemaphoreType.DMA
    third = (len(PARTS),)
    first = (*third, 2, 2, 3)
    second = (*third, 2, 3)
    return pl.pallas_call(
        functools.partial(kernel, rows, PARTS, ORDER, DIRECT),
        out_shape=vmem((CHUNKS * rows, TILE), jnp.float32),
        in_specs=[pl.BlockSpec(memory_space=pltpu.HBM)] * 4,
        out_specs=pl.BlockSpec(memory_space=vmem),
        scratch_shapes=[
            pltpu.SMEM(labels.shape, jnp.int32),
            pltpu.SMEM(slot_tile.shape, jnp.int32),
            vmem((CHUNKS, rows, depth), jnp.bfloat16),
            vmem((2, 4, 4, depth, 2 * TILE), jnp.bfloat16),
            vmem((CHUNKS, 2, 2, 4, 4, rows, TILE), jnp.float32),
            vmem((CHUNKS, 2, 4, 4, rows, TILE), jnp.float32),
            vmem((CHUNKS, 2, 4, rows, TILE), jnp.float32),
            vmem((CHUNKS, 2, rows, TILE), jnp.float32),
            vmem((*first, 2 * rows + 8, TILE), jnp.int16),
            vmem((*first, 2 * rows + 8, TILE), jnp.int16),
            vmem((*second, rows + 8, TILE), jnp.int16),
            vmem((*second, rows + 8, TILE), jnp.int16),
            vmem((*third, rows + 8, TILE), jnp.int16),
            vmem((*third, rows + 8, TILE), jnp.int16),
            dma((3,)), dma((2, 4)), pltpu.SemaphoreType.REGULAR, dma, dma((CHUNKS,)), dma((CHUNKS,)), dma((CHUNKS, 4)),
            dma(third), dma((*third, 2, 2)), dma(third), dma((*third, 2, 2)), dma(third), dma(third),
        ],
        compiler_params=pltpu.CompilerParams(
            collective_id=0, has_side_effects=True, vmem_limit_bytes=60 * 1024 * 1024
        ),
        name="ladder",
    )(amplitudes, integrals, labels, slot_tile)


def solution(mesh):
    split = Mesh(
        mesh.devices.reshape(mesh.shape["occ"], 4, 4, 2, 2),
        ("occ", "vir_0", "vir_1", "vir_2", "vir_3"),
    )
    placed = (P("occ", VIR), P(VIR, "occ"), P(), P())
    return jax.shard_map(
        shards, mesh=split, in_specs=placed, out_specs=P(None, OCC_VIR), check_vma=False
    )
```
